32 devices in a mesh: grp: 2 (over y), freq: 4 (over z), beam: 2 (over x), dm: 2 (over core).
Axes of the slice: x: 2, y: 2, z: 4, core: 2. Of those that a mesh axis runs over, the one named last changes fastest.
Arguments:
- voltages: bfloat16 [4, 2048, 16, 2, 1024], P(None, ('freq', 'beam'), ('grp', 'dm')), parts along dimension 2, may hold values from -6 to 6
- grid_feed: int32 [1024], replicated, may hold values from 0 to 1023, each once
- delays: int32 [4, 2048, 256], P('freq', None, 'dm'), may hold values from 0 to 4
Outputs:
- dedispersed: float32 [4, 256, 8, 1024], P('freq', 'dm', 'grp', 'beam'), parts along dimension 2
The draws below stay inside these ranges and needn't reach their ends.
There are 2 independent parts, one for each index of `grp`. The reference program is written for one: setup_inputs(seed, part) draws one part's arguments, and reference() takes and returns one part's arrays. A program takes and returns all parts, laid end to end along the dimension named above; an argument that names none is the same for every part. Nothing has to cross between parts.
Inputs may be any that keep to these rules, and one draw needn't show every extreme that they name: `grid_feed`: each feed appears once.
All inputs are finite; a program needn't handle non-finite values.
Results may differ from the reference program's by a relative error of at most 0.0034.
Values may be sent and summed in bfloat16 or wider, within the bound.
A program may use at most 128 MiB of HBM per device.

```python
import math
import jax
import jax.numpy as jnp
from jax import lax

GX = 4
GY = 256
FEEDS = 1024
FREQS = 8192
DMS = 256
TIME = 8
TOUT = 4
NBAND = 4
SUBS = 2048


def draw_delays(key, part):
    deepest = TIME - TOUT
    channels = NBAND * SUBS
    key_value, key_jitter, key_place = jax.random.split(jax.random.fold_in(key, 7), 3)
    position = jnp.arange(channels, dtype=jnp.int32)
    lowered = 2 * channels - position
    quotient = 4 * channels * channels // lowered
    weight = quotient * 1024 // lowered - 1024
    heaviest = jnp.max(weight)
    trial_value = jax.random.randint(key_value, (DMS,), 0, deepest + 1, dtype=jnp.int32)
    forced_dm = jax.random.randint(key_place, (), 0, DMS, dtype=jnp.int32)
    trial_value = jnp.where(jnp.arange(DMS, dtype=jnp.int32) == forced_dm, deepest, trial_value)
    base_delay = trial_value[None, :] * weight[:, None] // heaviest
    jitter = jax.random.randint(key_jitter, (channels, DMS), 0, 2, dtype=jnp.int32)
    return jnp.minimum(base_delay + jitter, deepest).reshape(NBAND, SUBS, DMS).astype(jnp.int32)


def shard_levels(stream_key, shape, cuts, smallest, top_value):
    def one(dim, shards_of):
        heights = jax.random.uniform(jax.random.fold_in(jax.random.fold_in(stream_key, 6), dim), (shards_of,), jnp.float32, smallest / len(cuts), top_value / len(cuts))
        return jnp.repeat(jnp.exp(heights), shape[dim] // shards_of).reshape((-1,) + (1,) * (len(shape) - dim - 1))

    loudness = one(*cuts[0])
    for cut in cuts[1:]:
        loudness = loudness * one(*cut)
    return loudness


def gaussian(rng, shape, spread, bound, cuts=(), kind=jnp.bfloat16):
    loudness = shard_levels(rng, shape, cuts, -0.22, 0.18) if cuts else 1.0
    array = jax.random.normal(rng, shape, jnp.float32) * spread * loudness
    return jnp.minimum(jnp.maximum(array, -bound), bound).astype(kind)


def setup_inputs(seed: int = 0, part: int = 0) -> dict:
    key_list = jax.random.split(jax.random.key(seed), 4)
    part_splits = jax.random.split(jax.random.fold_in(key_list[3], part), 4)
    return {
        "voltages": gaussian(part_splits[0], (NBAND, SUBS, TIME, 2, FEEDS), 1.0, 6.0, ((1, 8), (2, 2))),
        "grid_feed": jax.random.permutation(key_list[1], FEEDS).astype(jnp.int32),
        "delays": draw_delays(jax.random.fold_in(key_list[3], 71), part),
    }


def steering_table(length, factor):
    position = jnp.arange(length, dtype=jnp.int32)
    phase_step = position[:, None] * position[None, :] % length
    phase_angle = phase_step.astype(jnp.float32) * (2.0 * math.pi / length)
    cosine = jnp.cos(phase_angle) * factor
    sine_part = jnp.sin(phase_angle) * factor
    upper_half = jnp.concatenate([cosine, -sine_part], axis=1)
    lower_half = jnp.concatenate([sine_part, cosine], axis=1)
    return jnp.concatenate([upper_half, lower_half], axis=0).astype(jnp.bfloat16)

def quarter_table():
    position = jnp.arange(GX, dtype=jnp.int32)
    phase_step = position[:, None] * position[None, :] % GX
    cosine = jnp.where(phase_step == 0, 1.0, jnp.where(phase_step == 2, -1.0, 0.0)) * 0.5
    sine_part = jnp.where(phase_step == 1, 1.0, jnp.where(phase_step == 3, -1.0, 0.0)) * 0.5
    real_in = jnp.stack([cosine, -sine_part], axis=2)
    imag_in = jnp.stack([sine_part, cosine], axis=2)
    return jnp.stack([real_in, imag_in], axis=1).astype(jnp.float32)

def form_power(voltages, grid_feed):
    row_count = voltages.shape[0] * voltages.shape[1] * voltages.shape[2]
    feed_count = voltages.shape[4]
    gridded = jnp.take(voltages.reshape(row_count, 2, feed_count), grid_feed, axis=2)
    gridded = jnp.transpose(gridded.reshape(row_count, 2, GX, GY), (0, 2, 1, 3)).reshape(row_count * GX, 2 * GY)
    along_y = jnp.dot(gridded, steering_table(GY, 1.0 / math.sqrt(GY)), preferred_element_type=jnp.float32).astype(jnp.bfloat16)
    along_y = along_y.reshape(row_count, GX, 2, GY).astype(jnp.float32)
    formed = jnp.einsum('rgpy,gpbq->rbqy', along_y, quarter_table(), precision=lax.Precision.HIGHEST)
    intensity = 0.5 * (formed[:, :, 0, :] ** 2 + formed[:, :, 1, :] ** 2)
    return intensity.astype(jnp.bfloat16).reshape(row_count, feed_count)

def reference(voltages, grid_feed, delays):
    band_count, sub_count, total_time = (voltages.shape[0], voltages.shape[1], voltages.shape[2])
    feed_count = voltages.shape[4]
    dm_count = delays.shape[2]
    intensity = form_power(voltages, grid_feed).reshape(band_count, sub_count, total_time, feed_count)
    levels = intensity.astype(jnp.float32)
    centered = (levels - lax.optimization_barrier(jnp.mean(levels, axis=2, keepdims=True))).astype(jnp.bfloat16)
    out_time = total_time // 2
    offsets = jnp.arange(out_time, dtype=jnp.int32)
    factor = 1.0 / math.sqrt(FREQS)

    def one_channel(running, entries):
        channel_rows, lag_row = entries
        picked = jnp.take(channel_rows, lag_row[:, None] + offsets[None, :], axis=0)
        return (running + picked.astype(jnp.float32), None)

    def one_band(cumulative, entries):
        band_rows, band_lags = entries
        initial = jnp.zeros((dm_count, out_time, feed_count), jnp.float32)
        band_sum, _ = lax.scan(one_channel, initial, (band_rows, band_lags))
        cumulative = cumulative + band_sum
        return (cumulative, cumulative * factor)
    zeros_start = jnp.zeros((dm_count, out_time, feed_count), jnp.float32)
    _, outputs = lax.scan(one_band, zeros_start, (centered, delays))
    return outputs
```

```python
import functools
import math

import jax
import jax.numpy as jnp
import numpy as np
from jax import lax
from jax.experimental import pallas as pl
from jax.experimental.pallas import tpu as pltpu
from jax.sharding import PartitionSpec as P

GX = 4
GY = 256
FREQS = 8192
ROWS = 16
LAGS = 5
BEHIND = 5
MESH = pl.DeviceIdType.MESH


def steering_table(length, factor):
    position = jnp.arange(length, dtype=jnp.int32)
    phase_step = position[:, None] * position[None, :] % length
    phase_angle = phase_step.astype(jnp.float32) * (2.0 * math.pi / length)
    cosine = jnp.cos(phase_angle) * factor
    sine_part = jnp.sin(phase_angle) * factor
    upper_half = jnp.concatenate([cosine, -sine_part], axis=1)
    lower_half = jnp.concatenate([sine_part, cosine], axis=1)
    return jnp.concatenate([upper_half, lower_half], axis=0).astype(jnp.bfloat16)


def quarter_table():
    position = jnp.arange(GX, dtype=jnp.int32)
    phase_step = position[:, None] * position[None, :] % GX
    cosine = jnp.where(phase_step == 0, 1.0, jnp.where(phase_step == 2, -1.0, 0.0)) * 0.5
    sine_part = jnp.where(phase_step == 1, 1.0, jnp.where(phase_step == 3, -1.0, 0.0)) * 0.5
    real_in = jnp.stack([cosine, -sine_part], axis=2)
    imag_in = jnp.stack([sine_part, cosine], axis=2)
    return jnp.stack([real_in, imag_in], axis=1).astype(jnp.float32)


def form_power(voltages, grid_feed):
    row_count = voltages.shape[0] * voltages.shape[1] * voltages.shape[2]
    feed_count = voltages.shape[4]
    gridded = jnp.take(voltages.reshape(row_count, 2, feed_count), grid_feed, axis=2)
    gridded = jnp.transpose(gridded.reshape(row_count, 2, GX, GY), (0, 2, 1, 3)).reshape(
        row_count * GX, 2 * GY
    )
    along_y = jnp.dot(
        gridded, steering_table(GY, 1.0 / math.sqrt(GY)), preferred_element_type=jnp.float32
    ).astype(jnp.bfloat16)
    along_y = along_y.reshape(row_count, GX, 2, GY).astype(jnp.float32)
    formed = jnp.einsum(
        "rgpy,gpbq->rbqy", along_y, quarter_table(), precision=lax.Precision.HIGHEST
    )
    intensity = 0.5 * (formed[:, :, 0, :] ** 2 + formed[:, :, 1, :] ** 2)
    return intensity.astype(jnp.bfloat16).reshape(row_count, feed_count)


def regrouped_body(voltages, grid_feed, delays):
    band_count, sub_local, time_local = (voltages.shape[0], voltages.shape[1], voltages.shape[2])
    feed_count = voltages.shape[4]
    columns = lax.axis_size("beam")
    col_width = feed_count // columns
    intensity = form_power(voltages, grid_feed).reshape(
        band_count, sub_local, time_local, columns, col_width
    )
    regrouped = jnp.transpose(intensity, (0, 3, 1, 2, 4)).reshape(
        band_count * columns, sub_local, time_local, col_width
    )
    turned = lax.all_to_all(regrouped, ("freq", "beam"), split_axis=0, concat_axis=1, tiled=True)
    turned = turned.reshape(-1, time_local, col_width)
    full_time = lax.all_gather(turned, "dm", axis=1, tiled=True)
    sub_count, total_time = (full_time.shape[0], full_time.shape[1])
    levels = full_time.astype(jnp.float32)
    centered = (levels - jnp.mean(levels, axis=1, keepdims=True)).astype(jnp.bfloat16)
    flattened = centered.reshape(sub_count * total_time, col_width)
    out_time = total_time // 2
    offsets = jnp.arange(out_time, dtype=jnp.int32)
    sample_ids = jnp.arange(total_time, dtype=jnp.int32)
    dm_local = delays.shape[2]
    dm_block = 32
    lag_blocks = jnp.transpose(delays[0]).reshape(dm_local // dm_block, dm_block, sub_count)

    def dedisperse(lag_rows):
        shifted = offsets[None, :, None] + lag_rows[:, None, :]
        selector = (shifted[:, :, :, None] == sample_ids[None, None, None, :]).astype(jnp.bfloat16)
        summed = jnp.dot(
            selector.reshape(dm_block * out_time, sub_count * total_time),
            flattened,
            preferred_element_type=jnp.float32,
        )
        return summed.reshape(dm_block, out_time, col_width)

    partial_sum = lax.map(dedisperse, lag_blocks).reshape(dm_local, out_time, col_width)
    cumulative = lax.all_to_all(
        jnp.cumsum(
            lax.all_to_all(partial_sum[None], "freq", split_axis=1, concat_axis=0, tiled=True),
            axis=0,
        ),
        "freq",
        split_axis=0,
        concat_axis=1,
        tiled=True,
    )
    return cumulative * (1.0 / math.sqrt(FREQS))


def half_table():
    half = GY // 2
    cell = np.arange(GY)
    row = np.arange(half)
    angle = (cell[:, None] * row[None, :] % GY).astype(np.float32) * np.float32(2.0 * math.pi / GY)
    factor = np.float32(1.0 / math.sqrt(GY))
    sines = np.sin(angle) * factor
    sines[:, 0] = np.where(cell % 2 == 0, 1.0, -1.0) * factor
    table = np.concatenate([np.cos(angle) * factor, sines], axis=1)
    return jnp.asarray(table.astype(jnp.bfloat16))


def place_table(feed_ref, table_ref, full_ref):
    feeds = full_ref.shape[0]
    feed = lax.broadcasted_iota(jnp.int32, (feeds, GY), 0)
    for g in range(GX):
        cells = slice(g * GY, (g + 1) * GY)
        placed = jnp.where(feed == feed_ref[:, cells], 1.0, 0.0).astype(jnp.bfloat16)
        full_ref[:, cells] = jnp.dot(
            placed, table_ref[...], preferred_element_type=jnp.float32
        ).astype(jnp.bfloat16)


def beamform(volt_ref, full_ref, line_ref, level_ref):
    channels, feeds = volt_ref.shape[1], volt_ref.shape[4]
    half = GY // 2
    pairs = volt_ref[0, :, 0].reshape(2 * channels, feeds)
    for g in range(GX):
        line = jnp.dot(
            pairs, full_ref[:, g * GY : (g + 1) * GY], preferred_element_type=jnp.float32
        )
        line_ref[2 * g], line_ref[2 * g + 1] = line[:, :half], line[:, half:]
    first = lax.broadcasted_iota(jnp.int32, (ROWS, half), 1) == 0

    def rounded(a):
        return a.astype(jnp.bfloat16).astype(jnp.float32)

    for row in range(0, channels, ROWS):
        halves = ([], [])
        for g in range(GX):
            cos_r, sin_r, cos_i, sin_i = (
                line_ref[2 * g + h, pl.ds(2 * row + p, ROWS, stride=2), :]
                for p in range(2)
                for h in range(2)
            )
            odd_r, odd_i = jnp.where(first, 0.0, sin_r), jnp.where(first, 0.0, sin_i)
            halves[0].append((rounded(cos_r + odd_i), rounded(cos_i - odd_r)))
            even_r, even_i = jnp.where(first, sin_r, cos_r), jnp.where(first, sin_i, cos_i)
            halves[1].append((rounded(even_r - odd_i), rounded(even_i + odd_r)))
        for h, line in enumerate(halves):
            (r0, i0), (r1, i1), (r2, i2), (r3, i3) = line
            even_r, even_i, odd_r, odd_i = r0 + r2, i0 + i2, r1 + r3, i1 + i3
            diff_r, diff_i, turn_r, turn_i = r0 - r2, i0 - i2, i1 - i3, r3 - r1
            formed = (
                (even_r + odd_r, even_i + odd_i),
                (diff_r + turn_r, diff_i + turn_i),
                (even_r - odd_r, even_i - odd_i),
                (diff_r - turn_r, diff_i - turn_i),
            )
            for b, (re, im) in enumerate(formed):
                level_ref[row : row + ROWS, b * GY + h * half : b * GY + (h + 1) * half] = (
                    re * re + im * im
                ).astype(jnp.bfloat16)


def fused_kernel(
    bands,
    samples,
    feed_ref,
    table_ref,
    delay_ref,
    volt_ref,
    out_ref,
    full_ref,
    line_ref,
    level_ref,
    raw_ref,
    lag_out_ref,
    lag_ref,
    select_ref,
    mean_ref,
    total_ref,
    own_ref,
    beam_out_ref,
    beam_in_ref,
    band_out_ref,
    up_ref,
    down_ref,
    raw_sem,
    lag_sems,
    dm_sems,
    beam_sems,
    band_sem,
    up_sem,
    down_sem,
):
    me, column, core = lax.axis_index("freq"), lax.axis_index("beam"), lax.axis_index("dm")
    columns = lax.axis_size("beam")
    channels, feeds = volt_ref.shape[1], volt_ref.shape[4]
    trials = total_ref.shape[1]
    width = feeds // columns
    full_time = 2 * samples
    units = bands * samples
    step = pl.program_id(0)
    other_column, other_core = 1 - column, 1 - core

    def delay_copy(band):
        first = (band * columns + column) * channels
        return pltpu.make_async_copy(
            delay_ref.at[0, pl.ds(first, channels)], raw_ref.at[band], raw_sem.at[band]
        )

    def lag_copy(band):
        shift = lax.rem(band - me + bands, bands)
        return pltpu.make_async_remote_copy(
            src_ref=lag_out_ref.at[band],
            dst_ref=lag_ref.at[me],
            send_sem=lag_sems.at[0, shift],
            recv_sem=lag_sems.at[1, me],
            device_id={"freq": band},
            device_id_type=MESH,
        )

    def lag_arrival(band):
        return pltpu.make_async_remote_copy(
            src_ref=lag_out_ref.at[band],
            dst_ref=lag_ref.at[band],
            send_sem=lag_sems.at[0, 0],
            recv_sem=lag_sems.at[1, band],
            device_id={"freq": band},
            device_id_type=MESH,
        )

    def level_copy(band, sample, owner):
        return pltpu.make_async_remote_copy(
            src_ref=level_ref.at[band, owner * samples + sample],
            dst_ref=level_ref.at[band, owner * samples + sample],
            send_sem=dm_sems.at[0, band * samples + sample],
            recv_sem=dm_sems.at[1, band * samples + sample],
            device_id={"dm": other_core},
            device_id_type=MESH,
        )

    def beam_copy(unit):
        return pltpu.make_async_remote_copy(
            src_ref=beam_out_ref.at[unit],
            dst_ref=beam_in_ref.at[unit],
            send_sem=beam_sems.at[0, unit],
            recv_sem=beam_sems.at[1, unit],
            device_id={"beam": other_column},
            device_id_type=MESH,
        )

    def band_copy(unit, upward):
        return pltpu.make_async_remote_copy(
            src_ref=band_out_ref.at[unit],
            dst_ref=(up_ref if upward else down_ref).at[unit],
            send_sem=band_sem.at[unit],
            recv_sem=(up_sem if upward else down_sem).at[unit],
            device_id={"freq": me + 1 if upward else me - 1},
            device_id_type=MESH,
        )

    @pl.when(step == 0)
    def _():
        for band in range(bands):
            delay_copy(band).start()
        barrier = pltpu.get_barrier_semaphore()
        pl.semaphore_signal(barrier, inc=1, device_id={"dm": other_core}, device_id_type=MESH)
        pl.semaphore_signal(barrier, inc=1, device_id={"beam": other_column}, device_id_type=MESH)
        for shift in range(1, bands):
            pl.semaphore_signal(
                barrier,
                inc=1,
                device_id={"freq": lax.rem(me + shift, bands)},
                device_id_type=MESH,
            )
        for band in range(bands):
            delay_copy(band).wait()
            lag_out_ref[band] = raw_ref[band].astype(jnp.float32).T.astype(jnp.bfloat16)
        pl.semaphore_wait(barrier, bands + 1)
        for band in range(bands):

            @pl.when(band != me)
            def _():
                lag_copy(band).start()

        lag_ref[me] = lag_out_ref[me]
        total_ref[...] = jnp.zeros_like(total_ref)
        place_table(feed_ref, table_ref, full_ref)

    @pl.when(step < units)
    def _():
        band, sample = step // samples, lax.rem(step, samples)
        beamform(volt_ref, full_ref, line_ref, level_ref.at[band, core * samples + sample])
        level_copy(band, sample, core).start()

    @pl.when((step >= samples) & (step < samples + units))
    def _():
        unit = step - samples
        band, row = unit // samples, lax.rem(unit, samples)

        @pl.when(row == 0)
        def _():
            @pl.when(band != me)
            def _():
                lag_arrival(band).wait_recv()

            lag = lag_ref[band].astype(jnp.float32)
            for value in range(LAGS):
                select_ref[:, value * channels : (value + 1) * channels] = jnp.where(
                    lag == value, 1.0, 0.0
                ).astype(jnp.bfloat16)
            for sample in range(samples):
                level_copy(band, sample, other_core).wait_recv()
            share = jnp.full((ROWS, full_time * channels), 1.0 / full_time, jnp.bfloat16)
            for start in range(0, feeds, GY):
                mean_ref[:, start : start + GY] = jnp.dot(
                    share,
                    level_ref[band, :, :, start : start + GY].reshape(full_time * channels, GY),
                    preferred_element_type=jnp.float32,
                )[: mean_ref.shape[0]]

        for start in range(0, feeds, GY):
            cols = slice(start, start + GY)
            levels = level_ref[band, pl.ds(row, LAGS), :, cols].reshape(LAGS * channels, GY)
            summed = jnp.dot(select_ref[...], levels, preferred_element_type=jnp.float32)
            total_ref[row, :, cols] += summed - mean_ref[:1, cols]
        away = pl.multiple_of(other_column * width, width)
        here = pl.multiple_of(column * width, width)
        beam_out_ref[unit] = total_ref[row, :, pl.ds(away, width)].astype(jnp.bfloat16)
        own_ref[unit] = total_ref[row, :, pl.ds(here, width)]
        beam_copy(unit).start()
        level_copy(band, row, core).wait_send()

    @pl.when(step >= samples + BEHIND)
    def _():
        unit = step - samples - BEHIND
        band, row = unit // samples, lax.rem(unit, samples)
        beam_copy(unit).wait()
        own_ref[unit] += beam_in_ref[unit].astype(jnp.float32)

        @pl.when((me > 0) & (me <= band))
        def _():
            band_copy(unit, True).wait_recv()
            own_ref[unit] += up_ref[unit].astype(jnp.float32)

        @pl.when((me < bands - 1) & (me >= band))
        def _():
            band_copy(unit, False).wait_recv()
            own_ref[unit] += down_ref[unit].astype(jnp.float32)

        @pl.when(me != band)
        def _():
            band_out_ref[unit] = own_ref[unit].astype(jnp.bfloat16)

        @pl.when(me < band)
        def _():
            band_copy(unit, True).start()

        @pl.when(me > band)
        def _():
            band_copy(unit, False).start()

        @pl.when(me == band)
        def _():
            half = GY // 2
            lane = lax.broadcasted_iota(jnp.int32, (trials, half), 1)
            back = jnp.where(lane == 0, 0, half - lane)
            factor = 0.125 / math.sqrt(FREQS)
            for start in range(0, width, half):
                part = own_ref[unit, :, start : start + half] * factor
                if start % GY:
                    part = jnp.take_along_axis(part, back, axis=1)
                out_ref[row, :, start : start + half] = part

    @pl.when(step == pl.num_programs(0) - 1)
    def _():
        for band in range(bands):

            @pl.when(band != me)
            def _():
                lag_copy(band).wait_send()

        for unit in range(units):

            @pl.when(unit // samples != me)
            def _():
                band_copy(unit, True).wait_send()


def fused(voltages, grid_feed, delays):
    bands, channels, samples, _, feeds = voltages.shape
    trials = delays.shape[2]
    width = feeds // lax.axis_size("beam")
    units = bands * samples
    vmem, dma = pltpu.VMEM, pltpu.SemaphoreType.DMA

    def block(step):
        step = jnp.minimum(step, units - 1)
        return (step // samples, 0, lax.rem(step, samples), 0, 0)

    return pl.pallas_call(
        functools.partial(fused_kernel, bands, samples),
        grid=(units + samples + BEHIND,),
        in_specs=[
            pl.BlockSpec((1, feeds), lambda i: (0, 0)),
            pl.BlockSpec((GY, GY), lambda i: (0, 0)),
            pl.BlockSpec(memory_space=pl.ANY),
            pl.BlockSpec((1, channels, 1, 2, feeds), block),
        ],
        out_specs=pl.BlockSpec((samples, trials, width), lambda i: (0, 0, 0)),
        out_shape=jax.ShapeDtypeStruct((samples, trials, width), jnp.float32),
        scratch_shapes=[
            vmem((feeds, feeds), jnp.bfloat16),
            vmem((2 * GX, 2 * channels, GY // 2), jnp.float32),
            vmem((bands, 2 * samples, channels, feeds), jnp.bfloat16),
            vmem((bands, channels, trials), jnp.int32),
            vmem((bands, trials, channels), jnp.bfloat16),
            vmem((bands, trials, channels), jnp.bfloat16),
            vmem((trials, LAGS * channels), jnp.bfloat16),
            vmem((8, feeds), jnp.float32),
            vmem((samples, trials, feeds), jnp.float32),
            vmem((units, trials, width), jnp.float32),
            vmem((units, trials, width), jnp.bfloat16),
            vmem((units, trials, width), jnp.bfloat16),
            vmem((units, trials, width), jnp.bfloat16),
            vmem((units, trials, width), jnp.bfloat16),
            vmem((units, trials, width), jnp.bfloat16),
            dma((bands,)),
            dma((2, bands)),
            dma((2, units)),
            dma((2, units)),
            dma((units,)),
            dma((units,)),
            dma((units,)),
        ],
        compiler_params=pltpu.CompilerParams(
            collective_id=0, has_side_effects=True, vmem_limit_bytes=63 * 2**20
        ),
    )(grid_feed.reshape(1, feeds), half_table(), delays, voltages)


def body(voltages, grid_feed, delays):
    bands, channels, samples = voltages.shape[0], voltages.shape[1], voltages.shape[2]
    feeds = voltages.shape[4]
    fits = (
        channels == 256
        and feeds == GX * GY
        and delays.shape[0] == 1
        and delays.shape[2] == 128
        and samples + 1 == LAGS
        and bands == lax.axis_size("freq")
        and lax.axis_size("beam") == 2
        and lax.axis_size("dm") == 2
    )
    if not fits:
        return regrouped_body(voltages, grid_feed, delays)
    return jnp.transpose(fused(voltages, grid_feed, delays), (1, 0, 2))[None]


def solution(mesh):
    in_specs = (P(None, ("freq", "beam"), ("grp", "dm"), None, None), P(), P("freq", None, "dm"))
    out_specs = P("freq", "dm", "grp", "beam")
    return jax.shard_map(body, mesh=mesh, in_specs=in_specs, out_specs=out_specs, check_vma=False)
```

```python
import functools
import math

import jax
import jax.numpy as jnp
import numpy as np
from jax import lax
from jax.experimental import pallas as pl
from jax.experimental.pallas import tpu as pltpu
from jax.sharding import PartitionSpec as P

GX = 4
GY = 256
FREQS = 8192
ROWS = 16
LAGS = 5
HOP = 2
SLOTS = 4
PIECES = 2
MESH = pl.DeviceIdType.MESH


def steering_table(length, factor):
    position = jnp.arange(length, dtype=jnp.int32)
    phase_step = position[:, None] * position[None, :] % length
    phase_angle = phase_step.astype(jnp.float32) * (2.0 * math.pi / length)
    cosine = jnp.cos(phase_angle) * factor
    sine_part = jnp.sin(phase_angle) * factor
    upper_half = jnp.concatenate([cosine, -sine_part], axis=1)
    lower_half = jnp.concatenate([sine_part, cosine], axis=1)
    return jnp.concatenate([upper_half, lower_half], axis=0).astype(jnp.bfloat16)


def quarter_table():
    position = jnp.arange(GX, dtype=jnp.int32)
    phase_step = position[:, None] * position[None, :] % GX
    cosine = jnp.where(phase_step == 0, 1.0, jnp.where(phase_step == 2, -1.0, 0.0)) * 0.5
    sine_part = jnp.where(phase_step == 1, 1.0, jnp.where(phase_step == 3, -1.0, 0.0)) * 0.5
    real_in = jnp.stack([cosine, -sine_part], axis=2)
    imag_in = jnp.stack([sine_part, cosine], axis=2)
    return jnp.stack([real_in, imag_in], axis=1).astype(jnp.float32)


def form_power(voltages, grid_feed):
    row_count = voltages.shape[0] * voltages.shape[1] * voltages.shape[2]
    feed_count = voltages.shape[4]
    gridded = jnp.take(voltages.reshape(row_count, 2, feed_count), grid_feed, axis=2)
    gridded = jnp.transpose(gridded.reshape(row_count, 2, GX, GY), (0, 2, 1, 3)).reshape(
        row_count * GX, 2 * GY
    )
    along_y = jnp.dot(
        gridded, steering_table(GY, 1.0 / math.sqrt(GY)), preferred_element_type=jnp.float32
    ).astype(jnp.bfloat16)
    along_y = along_y.reshape(row_count, GX, 2, GY).astype(jnp.float32)
    formed = jnp.einsum(
        "rgpy,gpbq->rbqy", along_y, quarter_table(), precision=lax.Precision.HIGHEST
    )
    intensity = 0.5 * (formed[:, :, 0, :] ** 2 + formed[:, :, 1, :] ** 2)
    return intensity.astype(jnp.bfloat16).reshape(row_count, feed_count)


def regrouped_body(voltages, grid_feed, delays):
    band_count, sub_local, time_local = (voltages.shape[0], voltages.shape[1], voltages.shape[2])
    feed_count = voltages.shape[4]
    columns = lax.axis_size("beam")
    col_width = feed_count // columns
    intensity = form_power(voltages, grid_feed).reshape(
        band_count, sub_local, time_local, columns, col_width
    )
    regrouped = jnp.transpose(intensity, (0, 3, 1, 2, 4)).reshape(
        band_count * columns, sub_local, time_local, col_width
    )
    turned = lax.all_to_all(regrouped, ("freq", "beam"), split_axis=0, concat_axis=1, tiled=True)
    turned = turned.reshape(-1, time_local, col_width)
    full_time = lax.all_gather(turned, "dm", axis=1, tiled=True)
    sub_count, total_time = (full_time.shape[0], full_time.shape[1])
    levels = full_time.astype(jnp.float32)
    centered = (levels - jnp.mean(levels, axis=1, keepdims=True)).astype(jnp.bfloat16)
    flattened = centered.reshape(sub_count * total_time, col_width)
    out_time = total_time // 2
    offsets = jnp.arange(out_time, dtype=jnp.int32)
    sample_ids = jnp.arange(total_time, dtype=jnp.int32)
    dm_local = delays.shape[2]
    dm_block = 32
    lag_blocks = jnp.transpose(delays[0]).reshape(dm_local // dm_block, dm_block, sub_count)

    def dedisperse(lag_rows):
        shifted = offsets[None, :, None] + lag_rows[:, None, :]
        selector = (shifted[:, :, :, None] == sample_ids[None, None, None, :]).astype(jnp.bfloat16)
        summed = jnp.dot(
            selector.reshape(dm_block * out_time, sub_count * total_time),
            flattened,
            preferred_element_type=jnp.float32,
        )
        return summed.reshape(dm_block, out_time, col_width)

    partial_sum = lax.map(dedisperse, lag_blocks).reshape(dm_local, out_time, col_width)
    cumulative = lax.all_to_all(
        jnp.cumsum(
            lax.all_to_all(partial_sum[None], "freq", split_axis=1, concat_axis=0, tiled=True),
            axis=0,
        ),
        "freq",
        split_axis=0,
        concat_axis=1,
        tiled=True,
    )
    return cumulative * (1.0 / math.sqrt(FREQS))


def half_table():
    half = GY // 2
    cell = np.arange(GY)
    row = np.arange(half)
    angle = (cell[:, None] * row[None, :] % GY).astype(np.float32) * np.float32(2.0 * math.pi / GY)
    factor = np.float32(1.0 / math.sqrt(GY))
    sines = np.sin(angle) * factor
    sines[:, 0] = np.where(cell % 2 == 0, 1.0, -1.0) * factor
    table = np.concatenate([np.cos(angle) * factor, sines], axis=1)
    return jnp.asarray(table.astype(jnp.bfloat16))


def place_table(feed_ref, table_ref, full_ref):
    feeds = full_ref.shape[0]
    feed = lax.broadcasted_iota(jnp.int32, (feeds, GY), 0)

    @pl.loop(0, GX)
    def _(g):
        cells = pl.ds(pl.multiple_of(g * GY, GY), GY)
        placed = jnp.where(feed == feed_ref[:, cells], 1.0, 0.0).astype(jnp.bfloat16)
        full_ref[:, cells] = jnp.dot(
            placed, table_ref[...], preferred_element_type=jnp.float32
        ).astype(jnp.bfloat16)


def transform_y(pairs_ref, full_ref, line_ref, g):
    channels, _, feeds = pairs_ref.shape
    line = jnp.dot(
        pairs_ref[...].reshape(2 * channels, feeds),
        full_ref[:, g * GY : (g + 1) * GY],
        preferred_element_type=jnp.float32,
    )
    line_ref[2 * g], line_ref[2 * g + 1] = line[:, : GY // 2], line[:, GY // 2 :]


def transform_x(line_ref, level_ref, row):
    half = GY // 2
    first = lax.broadcasted_iota(jnp.int32, (ROWS, half), 1) == 0

    def rounded(a):
        return a.astype(jnp.bfloat16).astype(jnp.float32)

    halves = ([], [])
    for g in range(GX):
        cos_r, sin_r, cos_i, sin_i = (
            line_ref[2 * g + h, pl.ds(2 * row + p, ROWS, stride=2), :]
            for p in range(2)
            for h in range(2)
        )
        odd_r, odd_i = jnp.where(first, 0.0, sin_r), jnp.where(first, 0.0, sin_i)
        halves[0].append((rounded(cos_r + odd_i), rounded(cos_i - odd_r)))
        even_r, even_i = jnp.where(first, sin_r, cos_r), jnp.where(first, sin_i, cos_i)
        halves[1].append((rounded(even_r - odd_i), rounded(even_i + odd_r)))
    for h, line in enumerate(halves):
        (r0, i0), (r1, i1), (r2, i2), (r3, i3) = line
        even_r, even_i, odd_r, odd_i = r0 + r2, i0 + i2, r1 + r3, i1 + i3
        diff_r, diff_i, turn_r, turn_i = r0 - r2, i0 - i2, i1 - i3, r3 - r1
        formed = (
            (even_r + odd_r, even_i + odd_i),
            (diff_r + turn_r, diff_i + turn_i),
            (even_r - odd_r, even_i - odd_i),
            (diff_r - turn_r, diff_i - turn_i),
        )
        for b, (re, im) in enumerate(formed):
            level_ref[row : row + ROWS, b * GY + h * half : b * GY + (h + 1) * half] = (
                re * re + im * im
            ).astype(jnp.bfloat16)


def send_order(bands, samples):
    units = [(0, 0), (1, 0), (1, 1), (1, 2), (0, 1), (2, 0), (2, 1), (0, 2), (0, 3)]
    units += [(3, row) for row in range(samples)] + [(2, 2), (2, 3), (1, 3)]
    return [band * samples + row for band, row in units]


def fused_kernel(
    bands,
    samples,
    feed_ref,
    table_ref,
    delay_ref,
    volt_ref,
    out_ref,
    full_ref,
    held_ref,
    line0_ref,
    line1_ref,
    level_ref,
    raw_ref,
    lag_out_ref,
    lag_ref,
    select_ref,
    mean_ref,
    total_ref,
    own_ref,
    beam_out_ref,
    beam_in_ref,
    band_out_ref,
    up_ref,
    down_ref,
    volt_sem,
    raw_sem,
    lag_sems,
    dm_sems,
    beam_sems,
    band_sem,
    up_sem,
    down_sem,
):
    me, column, core = lax.axis_index("freq"), lax.axis_index("beam"), lax.axis_index("dm")
    columns = lax.axis_size("beam")
    channels, feeds = volt_ref.shape[1], volt_ref.shape[4]
    slots, part = held_ref.shape[0], channels // 2
    trials = total_ref.shape[1]
    width = feeds // columns
    full_time = 2 * samples
    units = bands * samples
    other_column, other_core = 1 - column, 1 - core

    def rows_of(piece):
        return slice(piece * trials // PIECES, (piece + 1) * trials // PIECES)

    order = send_order(bands, samples)

    def unit_at(place):
        found = jnp.int32(order[0])
        for at, unit in enumerate(order[1:]):
            found = jnp.where(place > at, unit, found)
        return found

    def delay_copy(band):
        first = (band * columns + column) * channels
        return pltpu.make_async_copy(
            delay_ref.at[0, pl.ds(first, channels)], raw_ref.at[band], raw_sem.at[band]
        )

    def lag_copy(band):
        shift = lax.rem(band - me + bands, bands)
        return pltpu.make_async_remote_copy(
            src_ref=lag_out_ref.at[band],
            dst_ref=lag_ref.at[me],
            send_sem=lag_sems.at[0, shift],
            recv_sem=lag_sems.at[1, me],
            device_id={"freq": band},
            device_id_type=MESH,
        )

    def lag_arrival(band):
        return pltpu.make_async_remote_copy(
            src_ref=lag_out_ref.at[band],
            dst_ref=lag_ref.at[band],
            send_sem=lag_sems.at[0, 0],
            recv_sem=lag_sems.at[1, band],
            device_id={"freq": band},
            device_id_type=MESH,
        )

    def level_copy(band, sample, owner):
        return pltpu.make_async_remote_copy(
            src_ref=level_ref.at[band, owner * samples + sample],
            dst_ref=level_ref.at[band, owner * samples + sample],
            send_sem=dm_sems.at[0, band * samples + sample],
            recv_sem=dm_sems.at[1, band * samples + sample],
            device_id={"dm": other_core},
            device_id_type=MESH,
        )

    def beam_copy(unit, piece):
        return pltpu.make_async_remote_copy(
            src_ref=beam_out_ref.at[unit, rows_of(piece)],
            dst_ref=beam_in_ref.at[unit, rows_of(piece)],
            send_sem=beam_sems.at[0, unit * PIECES + piece],
            recv_sem=beam_sems.at[1, unit * PIECES + piece],
            device_id={"beam": other_column},
            device_id_type=MESH,
        )

    def band_copy(unit, piece, upward):
        return pltpu.make_async_remote_copy(
            src_ref=band_out_ref.at[unit, rows_of(piece)],
            dst_ref=(up_ref if upward else down_ref).at[unit, rows_of(piece)],
            send_sem=band_sem.at[unit * PIECES + piece],
            recv_sem=(up_sem if upward else down_sem).at[unit * PIECES + piece],
            device_id={"freq": me + 1 if upward else me - 1},
            device_id_type=MESH,
        )

    def volt_copy(step):
        band, sample, slot = step // samples, lax.rem(step, samples), lax.rem(step, slots)
        return pltpu.make_async_copy(
            volt_ref.at[band, :, sample], held_ref.at[slot], volt_sem.at[slot]
        )

    def enter():
        for band in range(bands):
            delay_copy(band).start()
        for step in range(slots - 1):
            volt_copy(step).start()
        barrier = pltpu.get_barrier_semaphore()
        pl.semaphore_signal(barrier, inc=1, device_id={"dm": other_core}, device_id_type=MESH)
        pl.semaphore_signal(barrier, inc=1, device_id={"beam": other_column}, device_id_type=MESH)
        for shift in range(1, bands):
            pl.semaphore_signal(
                barrier,
                inc=1,
                device_id={"freq": lax.rem(me + shift, bands)},
                device_id_type=MESH,
            )
        place_table(feed_ref, table_ref, full_ref)

    def share_lags():
        @pl.loop(0, bands)
        def _(band):
            delay_copy(band).wait()
            lag_out_ref[band] = raw_ref[band].astype(jnp.float32).T.astype(jnp.bfloat16)
        pl.semaphore_wait(pltpu.get_barrier_semaphore(), bands + 1)
        for band in reversed(range(bands)):

            @pl.when(band != me)
            def _():
                lag_copy(band).start()

        lag_ref[me] = lag_out_ref[me]
        total_ref[...] = jnp.zeros_like(total_ref)

    def form_beams(step):
        band, sample = step // samples, lax.rem(step, samples)
        levels_ref = level_ref.at[band, core * samples + sample]
        volt_copy(step).wait()

        @pl.when(step + slots - 1 < units)
        def _():
            volt_copy(step + slots - 1).start()

        block_ref = held_ref.at[lax.rem(step, slots)]
        rows = range(0, part, ROWS)
        for g in range(GX):
            transform_y(block_ref.at[:part], full_ref, line0_ref, g)
        for g in range(GX):
            transform_y(block_ref.at[part:], full_ref, line1_ref, g)
            for row in rows[g::GX]:
                transform_x(line0_ref, levels_ref.at[:part], row)
        for row in rows:
            transform_x(line1_ref, levels_ref.at[part:], row)

        @pl.when(step == 0)
        def _():
            share_lags()

        level_copy(band, sample, core).start()

    def prepare(band):
        @pl.when(band != me)
        def _():
            lag_arrival(band).wait_recv()

        lag = lag_ref[band].astype(jnp.float32)
        for value in range(LAGS):
            select_ref[:, value * channels : (value + 1) * channels] = jnp.where(
                lag == value, 1.0, 0.0
            ).astype(jnp.bfloat16)
        for sample in range(samples):
            level_copy(band, sample, other_core).wait_recv()
        share = jnp.full((ROWS, full_time * channels), 1.0 / full_time, jnp.bfloat16)
        for start in range(0, feeds, GY):
            mean_ref[:, start : start + GY] = jnp.dot(
                share,
                level_ref[band, :, :, start : start + GY].reshape(full_time * channels, GY),
                preferred_element_type=jnp.float32,
            )[: mean_ref.shape[0]]

    def sum_channels(unit):
        band, row = unit // samples, lax.rem(unit, samples)
        for g in range(GX):
            cols = slice(g * GY, (g + 1) * GY)
            levels = level_ref[band, pl.ds(row, LAGS), :, cols].reshape(LAGS * channels, GY)
            summed = jnp.dot(select_ref[...], levels, preferred_element_type=jnp.float32)
            total_ref[row, :, cols] += summed - mean_ref[:1, cols]
        away = pl.multiple_of(other_column * width, width)
        here = pl.multiple_of(column * width, width)
        beam_out_ref[unit] = total_ref[row, :, pl.ds(away, width)].astype(jnp.bfloat16)
        own_ref[unit] = total_ref[row, :, pl.ds(here, width)]
        level_copy(band, row, core).wait_send()

    def send_sums(unit):
        for piece in range(PIECES):
            beam_copy(unit, piece).start()

    def forward(unit, piece, upward):
        rows = rows_of(piece)
        band_out_ref[unit, rows] = own_ref[unit, rows].astype(jnp.bfloat16)
        band_copy(unit, piece, upward).start()

    def arrive(unit, piece, upward):
        rows = rows_of(piece)
        band_copy(unit, piece, upward).wait_recv()
        own_ref[unit, rows] += (up_ref if upward else down_ref)[unit, rows].astype(jnp.float32)

    def links(place):
        @pl.when(place < units)
        def _():
            unit = unit_at(place)
            band = unit // samples
            for piece in range(PIECES):
                rows = rows_of(piece)
                beam_copy(unit, piece).wait()
                own_ref[unit, rows] += beam_in_ref[unit, rows].astype(jnp.float32)

                @pl.when((me == 0) & (band > 0))
                def _():
                    forward(unit, piece, True)

                @pl.when((me == bands - 1) & (band < me))
                def _():
                    forward(unit, piece, False)

        for upward in (True, False):
            hop = me if upward else bands - 1 - me
            earlier = place - HOP * hop
            unit = unit_at(jnp.maximum(earlier, 0))
            band = unit // samples
            beyond = band > me if upward else band < me

            @pl.when((hop > 0) & (earlier >= 0) & (earlier < units) & beyond)
            def _():
                for piece in range(PIECES):
                    arrive(unit, piece, upward)
                    forward(unit, piece, upward)

    def leave():
        half = GY // 2
        lane = lax.broadcasted_iota(jnp.int32, (trials, half), 1)
        back = jnp.where(lane == 0, 0, half - lane)
        factor = 0.125 / math.sqrt(FREQS)

        @pl.loop(0, samples)
        def _(row):
            unit = me * samples + row

            for piece in range(PIECES):

                @pl.when(me > 0)
                def _():
                    arrive(unit, piece, True)

                @pl.when(me < bands - 1)
                def _():
                    arrive(unit, piece, False)

            for start in range(0, width, half):
                part = own_ref[unit, :, start : start + half] * factor
                if start % GY:
                    part = jnp.take_along_axis(part, back, axis=1)
                out_ref[row, :, start : start + half] = part

        for band in range(bands):

            @pl.when(band != me)
            def _():
                lag_copy(band).wait_send()

        @pl.loop(0, units)
        def _(unit):
            @pl.when(unit // samples != me)
            def _():
                for piece in range(PIECES):
                    band_copy(unit, piece, True).wait_send()

    def form_band(band, place):
        @pl.loop(0, samples)
        def _(sample):
            form_beams(band * samples + sample)
            if place is not None:

                @pl.when(lax.rem(sample, 2) == 1)
                def _():
                    links(place + sample // 2)

    def sum_band(band, at_once):
        prepare(band)

        @pl.loop(0, samples)
        def _(row):
            sum_channels(band * samples + row)

            @pl.when(row < at_once)
            def _():
                send_sums(band * samples + row)

    def send_at(first, last):
        for unit in order[first:last]:
            send_sums(unit)

    enter()

    @pl.loop(0, 2 * samples)
    def _(step):
        form_beams(step)

    sum_band(0, 1)
    sum_band(1, 3)
    send_at(4, 5)
    links(0)
    form_band(2, 1)
    sum_band(2, 2)
    send_at(7, 9)
    links(3)
    form_band(3, 4)
    sum_band(3, samples)
    send_at(9 + samples, units)
    links(6)

    @pl.loop(7, units + HOP * (bands - 2))
    def _(place):
        links(place)

    leave()


def fused(voltages, grid_feed, delays):
    bands, channels, samples, _, feeds = voltages.shape
    trials = delays.shape[2]
    width = feeds // lax.axis_size("beam")
    units = bands * samples
    vmem, dma = pltpu.VMEM, pltpu.SemaphoreType.DMA

    return pl.pallas_call(
        functools.partial(fused_kernel, bands, samples),
        in_specs=[
            pl.BlockSpec(memory_space=vmem),
            pl.BlockSpec(memory_space=vmem),
            pl.BlockSpec(memory_space=pl.ANY),
            pl.BlockSpec(memory_space=pl.ANY),
        ],
        out_specs=pl.BlockSpec(memory_space=vmem),
        out_shape=jax.ShapeDtypeStruct((samples, trials, width), jnp.float32),
        scratch_shapes=[
            vmem((feeds, feeds), jnp.bfloat16),
            vmem((SLOTS, channels, 2, feeds), jnp.bfloat16),
            vmem((2 * GX, channels, GY // 2), jnp.float32),
            vmem((2 * GX, channels, GY // 2), jnp.float32),
            vmem((bands, 2 * samples, channels, feeds), jnp.bfloat16),
            vmem((bands, channels, trials), jnp.int32),
            vmem((bands, trials, channels), jnp.bfloat16),
            vmem((bands, trials, channels), jnp.bfloat16),
            vmem((trials, LAGS * channels), jnp.bfloat16),
            vmem((8, feeds), jnp.float32),
            vmem((samples, trials, feeds), jnp.float32),
            vmem((units, trials, width), jnp.float32),
            vmem((units, trials, width), jnp.bfloat16),
            vmem((units, trials, width), jnp.bfloat16),
            vmem((units, trials, width), jnp.bfloat16),
            vmem((units, trials, width), jnp.bfloat16),
            vmem((units, trials, width), jnp.bfloat16),
            dma((SLOTS,)),
            dma((bands,)),
            dma((2, bands)),
            dma((2, units)),
            dma((2, units * PIECES)),
            dma((units * PIECES,)),
            dma((units * PIECES,)),
            dma((units * PIECES,)),
        ],
        compiler_params=pltpu.CompilerParams(
            collective_id=0, has_side_effects=True, vmem_limit_bytes=63 * 2**20
        ),
    )(grid_feed.reshape(1, feeds), half_table(), delays, voltages)


def body(voltages, grid_feed, delays):
    bands, channels, samples = voltages.shape[0], voltages.shape[1], voltages.shape[2]
    feeds = voltages.shape[4]
    fits = (
        channels == 256
        and feeds == GX * GY
        and delays.shape[0] == 1
        and delays.shape[2] == 128
        and samples + 1 == LAGS
        and bands == 4
        and bands == lax.axis_size("freq")
        and lax.axis_size("beam") == 2
        and lax.axis_size("dm") == 2
    )
    if not fits:
        return regrouped_body(voltages, grid_feed, delays)
    return jnp.transpose(fused(voltages, grid_feed, delays), (1, 0, 2))[None]


def solution(mesh):
    in_specs = (P(None, ("freq", "beam"), ("grp", "dm"), None, None), P(), P("freq", None, "dm"))
    out_specs = P("freq", "dm", "grp", "beam")
    return jax.shard_map(body, mesh=mesh, in_specs=in_specs, out_specs=out_specs, check_vma=False)
```

```python
import functools
import math

import jax
import jax.numpy as jnp
import numpy as np
from jax import lax
from jax.experimental import pallas as pl
from jax.experimental.pallas import tpu as pltpu
from jax.sharding import PartitionSpec as P

GX = 4
GY = 256
FREQS = 8192
ROWS = 16
LAGS = 5
HOP = 2
SLOTS = 4
PIECES = 2
MESH = pl.DeviceIdType.MESH


def steering_table(length, factor):
    position = jnp.arange(length, dtype=jnp.int32)
    phase_step = position[:, None] * position[None, :] % length
    phase_angle = phase_step.astype(jnp.float32) * (2.0 * math.pi / length)
    cosine = jnp.cos(phase_angle) * factor
    sine_part = jnp.sin(phase_angle) * factor
    upper_half = jnp.concatenate([cosine, -sine_part], axis=1)
    lower_half = jnp.concatenate([sine_part, cosine], axis=1)
    return jnp.concatenate([upper_half, lower_half], axis=0).astype(jnp.bfloat16)


def quarter_table():
    position = jnp.arange(GX, dtype=jnp.int32)
    phase_step = position[:, None] * position[None, :] % GX
    cosine = jnp.where(phase_step == 0, 1.0, jnp.where(phase_step == 2, -1.0, 0.0)) * 0.5
    sine_part = jnp.where(phase_step == 1, 1.0, jnp.where(phase_step == 3, -1.0, 0.0)) * 0.5
    real_in = jnp.stack([cosine, -sine_part], axis=2)
    imag_in = jnp.stack([sine_part, cosine], axis=2)
    return jnp.stack([real_in, imag_in], axis=1).astype(jnp.float32)


def form_power(voltages, grid_feed):
    row_count = voltages.shape[0] * voltages.shape[1] * voltages.shape[2]
    feed_count = voltages.shape[4]
    gridded = jnp.take(voltages.reshape(row_count, 2, feed_count), grid_feed, axis=2)
    gridded = jnp.transpose(gridded.reshape(row_count, 2, GX, GY), (0, 2, 1, 3)).reshape(
        row_count * GX, 2 * GY
    )
    along_y = jnp.dot(
        gridded, steering_table(GY, 1.0 / math.sqrt(GY)), preferred_element_type=jnp.float32
    ).astype(jnp.bfloat16)
    along_y = along_y.reshape(row_count, GX, 2, GY).astype(jnp.float32)
    formed = jnp.einsum(
        "rgpy,gpbq->rbqy", along_y, quarter_table(), precision=lax.Precision.HIGHEST
    )
    intensity = 0.5 * (formed[:, :, 0, :] ** 2 + formed[:, :, 1, :] ** 2)
    return intensity.astype(jnp.bfloat16).reshape(row_count, feed_count)


def regrouped_body(voltages, grid_feed, delays):
    band_count, sub_local, time_local = (voltages.shape[0], voltages.shape[1], voltages.shape[2])
    feed_count = voltages.shape[4]
    columns = lax.axis_size("beam")
    col_width = feed_count // columns
    intensity = form_power(voltages, grid_feed).reshape(
        band_count, sub_local, time_local, columns, col_width
    )
    regrouped = jnp.transpose(intensity, (0, 3, 1, 2, 4)).reshape(
        band_count * columns, sub_local, time_local, col_width
    )
    turned = lax.all_to_all(regrouped, ("freq", "beam"), split_axis=0, concat_axis=1, tiled=True)
    turned = turned.reshape(-1, time_local, col_width)
    full_time = lax.all_gather(turned, "dm", axis=1, tiled=True)
    sub_count, total_time = (full_time.shape[0], full_time.shape[1])
    levels = full_time.astype(jnp.float32)
    centered = (levels - jnp.mean(levels, axis=1, keepdims=True)).astype(jnp.bfloat16)
    flattened = centered.reshape(sub_count * total_time, col_width)
    out_time = total_time // 2
    offsets = jnp.arange(out_time, dtype=jnp.int32)
    sample_ids = jnp.arange(total_time, dtype=jnp.int32)
    dm_local = delays.shape[2]
    dm_block = 32
    lag_blocks = jnp.transpose(delays[0]).reshape(dm_local // dm_block, dm_block, sub_count)

    def dedisperse(lag_rows):
        shifted = offsets[None, :, None] + lag_rows[:, None, :]
        selector = (shifted[:, :, :, None] == sample_ids[None, None, None, :]).astype(jnp.bfloat16)
        summed = jnp.dot(
            selector.reshape(dm_block * out_time, sub_count * total_time),
            flattened,
            preferred_element_type=jnp.float32,
        )
        return summed.reshape(dm_block, out_time, col_width)

    partial_sum = lax.map(dedisperse, lag_blocks).reshape(dm_local, out_time, col_width)
    cumulative = lax.all_to_all(
        jnp.cumsum(
            lax.all_to_all(partial_sum[None], "freq", split_axis=1, concat_axis=0, tiled=True),
            axis=0,
        ),
        "freq",
        split_axis=0,
        concat_axis=1,
        tiled=True,
    )
    return cumulative * (1.0 / math.sqrt(FREQS))


def half_table():
    half = GY // 2
    cell = np.arange(GY)
    row = np.arange(half)
    angle = (cell[:, None] * row[None, :] % GY).astype(np.float32) * np.float32(2.0 * math.pi / GY)
    factor = np.float32(1.0 / math.sqrt(GY))
    sines = np.sin(angle) * factor
    sines[:, 0] = np.where(cell % 2 == 0, 1.0, -1.0) * factor
    table = np.concatenate([np.cos(angle) * factor, sines], axis=1)
    return jnp.asarray(table.astype(jnp.bfloat16))


def place_table(feed_ref, table_ref, full_ref):
    feeds = full_ref.shape[0]
    feed = lax.broadcasted_iota(jnp.int32, (feeds, GY), 0)

    @pl.loop(0, GX)
    def _(g):
        cells = pl.ds(pl.multiple_of(g * GY, GY), GY)
        placed = jnp.where(feed == feed_ref[:, cells], 1.0, 0.0).astype(jnp.bfloat16)
        full_ref[:, cells] = jnp.dot(
            placed, table_ref[...], preferred_element_type=jnp.float32
        ).astype(jnp.bfloat16)


def transform_y(pairs_ref, full_ref, line_ref, g):
    channels, _, feeds = pairs_ref.shape
    line = jnp.dot(
        pairs_ref[...].reshape(2 * channels, feeds),
        full_ref[:, g * GY : (g + 1) * GY],
        preferred_element_type=jnp.float32,
    )
    line_ref[2 * g], line_ref[2 * g + 1] = line[:, : GY // 2], line[:, GY // 2 :]


def transform_x(line_ref, level_ref, row):
    half = GY // 2
    first = lax.broadcasted_iota(jnp.int32, (ROWS, half), 1) == 0

    def rounded(a):
        return a.astype(jnp.bfloat16).astype(jnp.float32)

    halves = ([], [])
    for g in range(GX):
        cos_r, sin_r, cos_i, sin_i = (
            line_ref[2 * g + h, pl.ds(2 * row + p, ROWS, stride=2), :]
            for p in range(2)
            for h in range(2)
        )
        odd_r, odd_i = jnp.where(first, 0.0, sin_r), jnp.where(first, 0.0, sin_i)
        halves[0].append((rounded(cos_r + odd_i), rounded(cos_i - odd_r)))
        even_r, even_i = jnp.where(first, sin_r, cos_r), jnp.where(first, sin_i, cos_i)
        halves[1].append((rounded(even_r - odd_i), rounded(even_i + odd_r)))
    for h, line in enumerate(halves):
        (r0, i0), (r1, i1), (r2, i2), (r3, i3) = line
        even_r, even_i, odd_r, odd_i = r0 + r2, i0 + i2, r1 + r3, i1 + i3
        diff_r, diff_i, turn_r, turn_i = r0 - r2, i0 - i2, i1 - i3, r3 - r1
        formed = (
            (even_r + odd_r, even_i + odd_i),
            (diff_r + turn_r, diff_i + turn_i),
            (even_r - odd_r, even_i - odd_i),
            (diff_r - turn_r, diff_i - turn_i),
        )
        for b, (re, im) in enumerate(formed):
            level_ref[row : row + ROWS, b * GY + h * half : b * GY + (h + 1) * half] = (
                re * re + im * im
            ).astype(jnp.bfloat16)


def send_order(bands, samples):
    units = [(0, 0), (1, 0), (1, 1), (1, 2), (0, 1), (2, 0), (2, 1), (0, 2), (0, 3)]
    units += [(3, row) for row in range(samples)] + [(2, 2), (2, 3), (1, 3)]
    return [band * samples + row for band, row in units]


def fused_kernel(
    bands,
    samples,
    feed_ref,
    table_ref,
    delay_ref,
    volt_ref,
    out_ref,
    full_ref,
    held_ref,
    line0_ref,
    line1_ref,
    level_ref,
    raw_ref,
    lag_out_ref,
    lag_ref,
    select_ref,
    mean_ref,
    total_ref,
    own_ref,
    beam_out_ref,
    beam_in_ref,
    band_out_ref,
    up_ref,
    down_ref,
    volt_sem,
    raw_sem,
    lag_sems,
    dm_sems,
    beam_sems,
    band_sem,
    up_sem,
    down_sem,
):
    me, column, core = lax.axis_index("freq"), lax.axis_index("beam"), lax.axis_index("dm")
    columns = lax.axis_size("beam")
    channels, feeds = volt_ref.shape[1], volt_ref.shape[4]
    slots, part = held_ref.shape[0], channels // 2
    trials = total_ref.shape[1]
    width = feeds // columns
    full_time = 2 * samples
    units = bands * samples
    other_column, other_core = 1 - column, 1 - core

    def rows_of(piece):
        return slice(piece * trials // PIECES, (piece + 1) * trials // PIECES)

    order = send_order(bands, samples)

    def unit_at(place):
        found = jnp.int32(order[0])
        for at, unit in enumerate(order[1:]):
            found = jnp.where(place > at, unit, found)
        return found

    def delay_copy(band):
        first = (band * columns + column) * channels
        return pltpu.make_async_copy(
            delay_ref.at[0, pl.ds(first, channels)], raw_ref.at[band], raw_sem.at[band]
        )

    def lag_copy(band):
        shift = lax.rem(band - me + bands, bands)
        return pltpu.make_async_remote_copy(
            src_ref=lag_out_ref.at[band],
            dst_ref=lag_ref.at[me],
            send_sem=lag_sems.at[0, shift],
            recv_sem=lag_sems.at[1, me],
            device_id={"freq": band},
            device_id_type=MESH,
        )

    def lag_arrival(band):
        return pltpu.make_async_remote_copy(
            src_ref=lag_out_ref.at[band],
            dst_ref=lag_ref.at[band],
            send_sem=lag_sems.at[0, 0],
            recv_sem=lag_sems.at[1, band],
            device_id={"freq": band},
            device_id_type=MESH,
        )

    def level_copy(band, sample, owner):
        return pltpu.make_async_remote_copy(
            src_ref=level_ref.at[band, owner * samples + sample],
            dst_ref=level_ref.at[band, owner * samples + sample],
            send_sem=dm_sems.at[0, band * samples + sample],
            recv_sem=dm_sems.at[1, band * samples + sample],
            device_id={"dm": other_core},
            device_id_type=MESH,
        )

    def beam_copy(unit, piece):
        return pltpu.make_async_remote_copy(
            src_ref=beam_out_ref.at[unit, rows_of(piece)],
            dst_ref=beam_in_ref.at[unit, rows_of(piece)],
            send_sem=beam_sems.at[0, unit * PIECES + piece],
            recv_sem=beam_sems.at[1, unit * PIECES + piece],
            device_id={"beam": other_column},
            device_id_type=MESH,
        )

    def band_copy(unit, piece, upward):
        return pltpu.make_async_remote_copy(
            src_ref=band_out_ref.at[unit, rows_of(piece)],
            dst_ref=(up_ref if upward else down_ref).at[unit, rows_of(piece)],
            send_sem=band_sem.at[unit * PIECES + piece],
            recv_sem=(up_sem if upward else down_sem).at[unit * PIECES + piece],
            device_id={"freq": me + 1 if upward else me - 1},
            device_id_type=MESH,
        )

    def volt_copy(step):
        band, sample, slot = step // samples, lax.rem(step, samples), lax.rem(step, slots)
        return pltpu.make_async_copy(
            volt_ref.at[band, :, sample], held_ref.at[slot], volt_sem.at[slot]
        )

    def enter():
        for band in range(bands):
            delay_copy(band).start()
        for step in range(slots - 1):
            volt_copy(step).start()
        barrier = pltpu.get_barrier_semaphore()
        pl.semaphore_signal(barrier, inc=1, device_id={"dm": other_core}, device_id_type=MESH)
        pl.semaphore_signal(barrier, inc=1, device_id={"beam": other_column}, device_id_type=MESH)
        for shift in range(1, bands):
            pl.semaphore_signal(
                barrier,
                inc=1,
                device_id={"freq": lax.rem(me + shift, bands)},
                device_id_type=MESH,
            )
        place_table(feed_ref, table_ref, full_ref)

    def share_lags():
        @pl.loop(0, bands)
        def _(band):
            delay_copy(band).wait()
            lag_out_ref[band] = raw_ref[band].astype(jnp.float32).T.astype(jnp.bfloat16)
        pl.semaphore_wait(pltpu.get_barrier_semaphore(), bands + 1)
        for band in reversed(range(bands)):

            @pl.when(band != me)
            def _():
                lag_copy(band).start()

        lag_ref[me] = lag_out_ref[me]
        total_ref[...] = jnp.zeros_like(total_ref)

    def form_beams(step):
        band, sample = step // samples, lax.rem(step, samples)
        levels_ref = level_ref.at[band, core * samples + sample]
        volt_copy(step).wait()

        @pl.when(step + slots - 1 < units)
        def _():
            volt_copy(step + slots - 1).start()

        block_ref = held_ref.at[lax.rem(step, slots)]
        rows = range(0, part, ROWS)
        for g in range(GX):
            transform_y(block_ref.at[:part], full_ref, line0_ref, g)
        for g in range(GX):
            transform_y(block_ref.at[part:], full_ref, line1_ref, g)
            for row in rows[g::GX]:
                transform_x(line0_ref, levels_ref.at[:part], row)
        for row in rows:
            transform_x(line1_ref, levels_ref.at[part:], row)

        @pl.when(step == 0)
        def _():
            share_lags()

        level_copy(band, sample, core).start()

    def prepare(band):
        @pl.when(band != me)
        def _():
            lag_arrival(band).wait_recv()

        lag = lag_ref[band].astype(jnp.float32)
        for value in range(LAGS):
            select_ref[:, value * channels : (value + 1) * channels] = jnp.where(
                lag == value, 1.0, 0.0
            ).astype(jnp.bfloat16)
        for sample in range(samples):
            level_copy(band, sample, other_core).wait_recv()
        share = jnp.full((ROWS, full_time * channels), 1.0 / full_time, jnp.bfloat16)
        for start in range(0, feeds, GY):
            mean_ref[:, start : start + GY] = jnp.dot(
                share,
                level_ref[band, :, :, start : start + GY].reshape(full_time * channels, GY),
                preferred_element_type=jnp.float32,
            )[: mean_ref.shape[0]]

    def sum_channels(unit):
        band, row = unit // samples, lax.rem(unit, samples)
        for g in range(GX):
            cols = slice(g * GY, (g + 1) * GY)
            levels = level_ref[band, pl.ds(row, LAGS), :, cols].reshape(LAGS * channels, GY)
            summed = jnp.dot(select_ref[...], levels, preferred_element_type=jnp.float32)
            total_ref[row, :, cols] += summed - mean_ref[:1, cols]
        away = pl.multiple_of(other_column * width, width)
        here = pl.multiple_of(column * width, width)
        beam_out_ref[unit] = total_ref[row, :, pl.ds(away, width)].astype(jnp.bfloat16)
        own_ref[unit] = total_ref[row, :, pl.ds(here, width)]
        level_copy(band, row, core).wait_send()

    def send_sums(unit):
        for piece in range(PIECES):
            beam_copy(unit, piece).start()

    def forward(unit, piece, upward):
        rows = rows_of(piece)
        band_out_ref[unit, rows] = own_ref[unit, rows].astype(jnp.bfloat16)
        band_copy(unit, piece, upward).start()

    def arrive(unit, piece, upward):
        rows = rows_of(piece)
        band_copy(unit, piece, upward).wait_recv()
        own_ref[unit, rows] += (up_ref if upward else down_ref)[unit, rows].astype(jnp.float32)

    def links(place):
        @pl.when(place < units)
        def _():
            unit = unit_at(place)
            band = unit // samples
            for piece in range(PIECES):
                rows = rows_of(piece)
                beam_copy(unit, piece).wait()
                own_ref[unit, rows] += beam_in_ref[unit, rows].astype(jnp.float32)

                @pl.when((me == 0) & (band > 0))
                def _():
                    forward(unit, piece, True)

                @pl.when((me == bands - 1) & (band < me))
                def _():
                    forward(unit, piece, False)

        for upward in (True, False):
            hop = me if upward else bands - 1 - me
            earlier = place - HOP * hop
            unit = unit_at(jnp.maximum(earlier, 0))
            band = unit // samples
            beyond = band > me if upward else band < me

            @pl.when((hop > 0) & (earlier >= 0) & (earlier < units) & beyond)
            def _():
                for piece in range(PIECES):
                    arrive(unit, piece, upward)
                    forward(unit, piece, upward)

    def leave():
        half = GY // 2
        lane = lax.broadcasted_iota(jnp.int32, (trials, half), 1)
        back = jnp.where(lane == 0, 0, half - lane)
        factor = 0.125 / math.sqrt(FREQS)

        for row in range(samples):
            unit = me * samples + row

            for piece in range(PIECES):

                @pl.when(me > 0)
                def _():
                    arrive(unit, piece, True)

                @pl.when(me < bands - 1)
                def _():
                    arrive(unit, piece, False)

            for start in range(0, width, half):
                part = own_ref[unit, :, start : start + half] * factor
                if start % GY:
                    part = jnp.take_along_axis(part, back, axis=1)
                out_ref[:, row, start : start + half] = part

        for band in range(bands):

            @pl.when(band != me)
            def _():
                lag_copy(band).wait_send()

        @pl.loop(0, units)
        def _(unit):
            @pl.when(unit // samples != me)
            def _():
                for piece in range(PIECES):
                    band_copy(unit, piece, True).wait_send()

    def form_band(band, place):
        @pl.loop(0, samples)
        def _(sample):
            form_beams(band * samples + sample)
            if place is not None:

                @pl.when(lax.rem(sample, 2) == 1)
                def _():
                    links(place + sample // 2)

    def sum_band(band, at_once):
        prepare(band)

        @pl.loop(0, samples)
        def _(row):
            sum_channels(band * samples + row)

            @pl.when(row < at_once)
            def _():
                send_sums(band * samples + row)

    def send_at(first, last):
        for unit in order[first:last]:
            send_sums(unit)

    enter()

    @pl.loop(0, 2 * samples)
    def _(step):
        form_beams(step)

    sum_band(0, 1)
    sum_band(1, 3)
    send_at(4, 5)
    links(0)
    form_band(2, 1)
    sum_band(2, 2)
    send_at(7, 9)
    links(3)
    form_band(3, 4)
    sum_band(3, samples)
    send_at(9 + samples, units)
    links(6)

    @pl.loop(7, units + HOP * (bands - 2))
    def _(place):
        links(place)

    leave()


def fused(voltages, grid_feed, delays):
    bands, channels, samples, _, feeds = voltages.shape
    trials = delays.shape[2]
    width = feeds // lax.axis_size("beam")
    units = bands * samples
    vmem, dma = pltpu.VMEM, pltpu.SemaphoreType.DMA

    return pl.pallas_call(
        functools.partial(fused_kernel, bands, samples),
        in_specs=[
            pl.BlockSpec(memory_space=vmem),
            pl.BlockSpec(memory_space=vmem),
            pl.BlockSpec(memory_space=pl.ANY),
            pl.BlockSpec(memory_space=pl.ANY),
        ],
        out_specs=pl.BlockSpec(memory_space=vmem),
        out_shape=jax.ShapeDtypeStruct((trials, samples, width), jnp.float32),
        scratch_shapes=[
            vmem((feeds, feeds), jnp.bfloat16),
            vmem((SLOTS, channels, 2, feeds), jnp.bfloat16),
            vmem((2 * GX, channels, GY // 2), jnp.float32),
            vmem((2 * GX, channels, GY // 2), jnp.float32),
            vmem((bands, 2 * samples, channels, feeds), jnp.bfloat16),
            vmem((bands, channels, trials), jnp.int32),
            vmem((bands, trials, channels), jnp.bfloat16),
            vmem((bands, trials, channels), jnp.bfloat16),
            vmem((trials, LAGS * channels), jnp.bfloat16),
            vmem((8, feeds), jnp.float32),
            vmem((samples, trials, feeds), jnp.float32),
            vmem((units, trials, width), jnp.float32),
            vmem((units, trials, width), jnp.bfloat16),
            vmem((units, trials, width), jnp.bfloat16),
            vmem((units, trials, width), jnp.bfloat16),
            vmem((units, trials, width), jnp.bfloat16),
            vmem((units, trials, width), jnp.bfloat16),
            dma((SLOTS,)),
            dma((bands,)),
            dma((2, bands)),
            dma((2, units)),
            dma((2, units * PIECES)),
            dma((units * PIECES,)),
            dma((units * PIECES,)),
            dma((units * PIECES,)),
        ],
        compiler_params=pltpu.CompilerParams(
            collective_id=0, has_side_effects=True, vmem_limit_bytes=63 * 2**20
        ),
    )(grid_feed.reshape(1, feeds), half_table(), delays, voltages)


def body(voltages, grid_feed, delays):
    bands, channels, samples = voltages.shape[0], voltages.shape[1], voltages.shape[2]
    feeds = voltages.shape[4]
    fits = (
        channels == 256
        and feeds == GX * GY
        and delays.shape[0] == 1
        and delays.shape[2] == 128
        and samples + 1 == LAGS
        and bands == 4
        and bands == lax.axis_size("freq")
        and lax.axis_size("beam") == 2
        and lax.axis_size("dm") == 2
    )
    if not fits:
        return regrouped_body(voltages, grid_feed, delays)
    return fused(voltages, grid_feed, delays)[None]


def solution(mesh):
    in_specs = (P(None, ("freq", "beam"), ("grp", "dm"), None, None), P(), P("freq", None, "dm"))
    out_specs = P("freq", "dm", "grp", "beam")
    return jax.shard_map(body, mesh=mesh, in_specs=in_specs, out_specs=out_specs, check_vma=False)
```
